128 devices in a mesh: row: 16 (over y, x_lo, core), col: 8 (over x_hi, z).
Axes of the slice: x: 4 (x_hi: 2, x_lo: 2; x = x_hi * 2 + x_lo), y: 4, z: 4, core: 2. Of those that a mesh axis runs over, the one named last changes fastest.
Arguments:
- lower_inverse: float32 [16, 8, 1024, 1024], P('row', 'col'), may hold values from -1 to 2, as said below
- upper_inverse: float32 [16, 8, 1024, 1024], P('row', 'col'), may hold values from -1 to 2, as said below
- left_coupling: bfloat16 [16, 8, 512, 1024], P('row', 'col'), may hold values from -0.1875 to 0.1875
- right_pieces: float32 [8, 1024, 2048], P('col', None, 'row'), may hold values from -6 to 6
- interface_block: int32 [16, 8, 4], P('row', 'col'), may hold values from 0 to 7, all different within a row
- a_gg: float32 [16, 1024, 2048], P('row', 'col'), may hold values from -6 to 6
- panel_order: int32 [16], replicated, may hold values from 0 to 15, each once
Outputs:
- schur: float32 [16, 1024, 2048], P('row', 'col')
The draws below stay inside these ranges and needn't reach their ends.
Inputs may be any that keep to these rules, and one draw needn't show every extreme that they name: `interface_block`: the 4 block ids of one subdomain are distinct. `panel_order`: A permutation of the column blocks. `lower_inverse`: lower triangular, diagonal between 1 and 2. `upper_inverse`: upper triangular, diagonal between 1 and 2.
All inputs are finite; a program needn't handle non-finite values.
Results may differ from the reference program's by a relative error of at most 0.0028.
Values sent between devices are 32-bit elements; how exact they have to be, the bound alone decides.
No kernel may reach another device: no remote copies, remote signals or barrier semaphores. Data moves between devices by JAX's collectives and lax.ppermute only.
A program may use at most 128 MiB of HBM per device.

```python
import jax
import jax.numpy as jnp
from jax import lax

NI = 1024
PW = 2048
WB = 128
KB = 4
PR = 1024
N_ROW = 16
N_COL = 8


def make_factor(key, below):
    first_key, second_key = jax.random.split(key)
    shape = (N_ROW, N_COL, NI, NI)
    spread = jnp.clip(jax.random.normal(first_key, shape, jnp.float32), -6.0, 6.0) * (0.5 / NI ** 0.5)
    diagonal = jax.random.uniform(second_key, (N_ROW, N_COL, NI), jnp.float32, 1.0, 2.0)
    rows = lax.broadcasted_iota(jnp.int32, (NI, NI), 0)
    cols = lax.broadcasted_iota(jnp.int32, (NI, NI), 1)
    if below:
        keep = rows > cols
    else:
        keep = rows < cols
    ones = (rows == cols).astype(jnp.float32)
    return jnp.where(keep, spread, 0.0) + diagonal[..., None] * ones


def draw_lower_inverse(key, part):
    return make_factor(jax.random.fold_in(key, 11), True)


def draw_upper_inverse(key, part):
    return make_factor(jax.random.fold_in(key, 23), False)


def steps_of(stream_key, shape, cuts, least, top_value):
    def one(dim, shards_of):
        steps = jax.random.uniform(jax.random.fold_in(jax.random.fold_in(stream_key, 6), dim), (shards_of,), jnp.float32, least / len(cuts), top_value / len(cuts))
        return jnp.repeat(jnp.exp(steps), shape[dim] // shards_of).reshape((-1,) + (1,) * (len(shape) - dim - 1))

    loudness = one(*cuts[0])
    for cut in cuts[1:]:
        loudness = loudness * one(*cut)
    return loudness


def different_ones(own_key, rows, number_of, top, lift):
    sequence = jax.random.permutation(jax.random.fold_in(own_key, 1), number_of)
    boost = sequence
    for power in range(3):
        boost = boost * boost // number_of
    boost = boost * lift // number_of
    tickets = jax.random.randint(jax.random.fold_in(own_key, 2), (rows, number_of), 0, 4096) + boost
    holders = jax.random.permutation(jax.random.fold_in(own_key, 3), rows)[jnp.arange(number_of) % rows]
    tickets = jnp.where(jnp.arange(rows)[:, None] == holders[None, :], 1 << 14, tickets)
    priority = tickets * number_of + jnp.arange(number_of)
    return lax.top_k(priority.astype(jnp.int32), top)[1].astype(jnp.int32)


def noise(stream_key, shape, scale, bound, cuts=(), held_as=jnp.bfloat16):
    array = scale * jax.random.normal(stream_key, shape, jnp.float32)
    if cuts:
        array = array * steps_of(stream_key, shape, cuts, -0.22, 0.18)
    return jnp.clip(array, -bound, bound).astype(held_as)


def setup_inputs(seed: int = 0) -> dict:
    streams_of = jax.random.split(jax.random.key(seed), 8)
    lower_inverse = draw_lower_inverse(jax.random.fold_in(streams_of[7], 71), 0)
    upper_inverse = draw_upper_inverse(jax.random.fold_in(streams_of[7], 71), 0)
    left_coupling = noise(streams_of[2], (N_ROW, N_COL, KB * WB, NI), NI ** -0.5, 0.1875, ((0, 16), (1, 8)))
    right_pieces = noise(streams_of[3], (N_COL, NI, PW), 1.0, 6.0, ((0, 8), (2, 16)), jnp.float32)
    interface_block = different_ones(streams_of[4], N_ROW * N_COL, N_COL, KB, 0).reshape((N_ROW, N_COL, KB))
    a_gg = noise(streams_of[5], (N_ROW, PR, PW), 1.0, 6.0, ((0, 16), (1, 8)), jnp.float32)
    panel_order = jax.random.permutation(streams_of[6], N_ROW).astype(jnp.int32)
    return {"lower_inverse": lower_inverse, "upper_inverse": upper_inverse, "left_coupling": left_coupling, "right_pieces": right_pieces, "interface_block": interface_block, "a_gg": a_gg, "panel_order": panel_order}


def column_order(panel_order):
    length = panel_order.shape[0]
    positions = jnp.arange(length, dtype=jnp.int32)
    hits = (panel_order[:, None] == positions[None, :]).astype(jnp.int32)
    return jnp.sum(hits * positions[:, None], axis=0).astype(jnp.int32)


def couple(lower_mat, upper_mat, left_mat, panel):
    halfway = jnp.dot(lower_mat, panel, precision=lax.Precision.HIGHEST, preferred_element_type=jnp.float32)
    solved = jnp.dot(upper_mat, halfway, precision=lax.Precision.HIGHEST, preferred_element_type=jnp.float32)
    solved = solved.astype(jnp.bfloat16)
    return jnp.dot(left_mat, solved, preferred_element_type=jnp.float32)


def place_rows(coupled, block_ids, first_block, block_total):
    block_count = block_ids.shape[0]
    block_rows = coupled.shape[0] // block_count
    targets = first_block + jnp.arange(block_total, dtype=jnp.int32)
    placed = (block_ids[:, None] == targets[None, :]).astype(jnp.float32)
    shaped = coupled.reshape(block_count, block_rows, coupled.shape[1])
    spread = jnp.einsum("kb,kwp->bwp", placed, shaped, precision=lax.Precision.HIGHEST)
    return spread.reshape(block_total * block_rows, coupled.shape[1])


def reference(lower_inverse, upper_inverse, left_coupling, right_pieces, interface_block, a_gg, panel_order):
    row_count = lower_inverse.shape[0]
    col_count = lower_inverse.shape[1]
    inner = right_pieces.shape[1]
    width_piece = right_pieces.shape[2] // row_count
    order = column_order(panel_order)
    panels = right_pieces.reshape(col_count, inner, row_count, width_piece)[:, :, order, :]
    panels = panels.reshape(col_count, inner, row_count * width_piece)

    def one_row(row_args):
        lowers, uppers, lefts, blocks, base = row_args

        def add_one(summed, item):
            lower_mat, upper_mat, left_mat, block_ids, panel = item
            coupled = couple(lower_mat, upper_mat, left_mat, panel)
            return summed + place_rows(coupled, block_ids, 0, col_count), None

        summed, _ = lax.scan(add_one, jnp.zeros(base.shape, jnp.float32), (lowers, uppers, lefts, blocks, panels))
        return base - summed

    return lax.map(one_row, (lower_inverse, upper_inverse, left_coupling, interface_block, a_gg))
```

```python
import jax
import jax.numpy as jnp
from jax import lax
from jax.experimental import pallas as pl
from jax.experimental.pallas import tpu as pltpu
from jax.sharding import PartitionSpec as P

F32 = jnp.float32
BF16 = jnp.bfloat16

CORE = [(r, r ^ 1) for r in range(16)]
XLO = [(r, r ^ 2) for r in range(16)]
XHI = [(c, c ^ 4) for c in range(8)]


def yshift(d):
    return [(r, ((r // 4 + d) % 4) * 4 + r % 4) for r in range(16)]


def zshift(d):
    return [(c, (c // 4) * 4 + (c % 4 + d) % 4) for c in range(8)]


def split(x):
    hi = x.astype(BF16)
    return hi, (x - hi.astype(F32)).astype(BF16)


def mm(a, b):
    return jnp.dot(a, b, preferred_element_type=F32)


VMEM = pl.BlockSpec(memory_space=pltpu.VMEM)
SMEM = pl.BlockSpec(memory_space=pltpu.SMEM)


def weights_kernel(steps, left_ref, upper_ref, lower_ref, whi_ref, wlo_ref, thi, tlo):
    step = pl.program_id(0)
    width = upper_ref.shape[1]
    for j in range(steps):

        @pl.when(step == j)
        def _(j=j):
            depth = (j + 1) * width
            uhi, ulo = split(upper_ref[0:depth, :])
            left = left_ref[:, 0:depth]
            t = mm(left, uhi) + mm(left, ulo)
            hi, lo = split(t)
            thi[:, j * width : (j + 1) * width] = hi
            tlo[:, j * width : (j + 1) * width] = lo

        @pl.when(step == steps + j)
        def _(j=j):
            lhi, llo = split(lower_ref[j * width :, :])
            ahi = thi[:, j * width :]
            w = mm(ahi, lhi) + mm(ahi, llo) + mm(tlo[:, j * width :], lhi)
            hi, lo = split(w)
            whi_ref[:, j * width : (j + 1) * width] = hi
            wlo_ref[:, j * width : (j + 1) * width] = lo


def weights(left, upper, lower):
    m, n = left.shape
    steps = 4
    width = n // steps
    shape = jax.ShapeDtypeStruct((m, n), BF16)
    return pl.pallas_call(
        lambda *refs: weights_kernel(steps, *refs),
        grid=(2 * steps,),
        in_specs=[
            pl.BlockSpec((m, n), lambda s: (0, 0)),
            pl.BlockSpec((n, width), lambda s: (0, jnp.minimum(s, steps - 1))),
            pl.BlockSpec((n, width), lambda s: (0, jnp.maximum(s - steps, 0))),
        ],
        out_specs=[pl.BlockSpec((m, n), lambda s: (0, 0))] * 2,
        out_shape=[shape, shape],
        scratch_shapes=[pltpu.VMEM((m, n), BF16)] * 2,
        cost_estimate=pl.CostEstimate(
            flops=6 * m * n * n, bytes_accessed=8 * n * n + 6 * m * n, transcendentals=0
        ),
        name="weights",
    )(left, upper, lower)


def couple_kernel(count, ids_ref, meta_ref, whi_ref, wlo_ref, *refs):
    pieces, outs, scratch = refs[:count], refs[count:-1], refs[-1]
    width = pieces[0].shape[1]
    his, los = zip(*(split(p[...]) for p in pieces))
    hi = jnp.concatenate(his, axis=1)
    lo = jnp.concatenate(los, axis=1)
    whi = whi_ref[...]
    scratch[...] = mm(whi, hi) + mm(whi, lo) + mm(wlo_ref[...], hi)
    col = meta_ref[1]
    x_hi, z = col // 4, col % 4
    for dx in range(2):
        for dz in range(4):
            out = outs[dx * 4 + dz]
            target = (x_hi + dx) % 2 * 4 + (z + dz) % 4
            source = jnp.int32(-1)
            for k in range(4):
                source = jnp.where(ids_ref[k] == target, jnp.int32(k), source)

            @pl.when(source >= 0)
            def _():
                rows = out.shape[0]
                out[...] = scratch[pl.ds(pl.multiple_of(source * rows, rows), rows), :]

            @pl.when(source < 0)
            def _():
                out[...] = jnp.zeros_like(out)


def couple(ids, meta, whi, wlo, pieces):
    m, k = whi.shape
    n = sum(p.shape[1] for p in pieces)
    shape = jax.ShapeDtypeStruct((m // 4, n), F32)
    return pl.pallas_call(
        lambda *refs: couple_kernel(len(pieces), *refs),
        in_specs=[SMEM, SMEM] + [VMEM] * (2 + len(pieces)),
        out_specs=[VMEM] * 8,
        out_shape=[shape] * 8,
        scratch_shapes=[pltpu.VMEM((m, n), F32)],
        cost_estimate=pl.CostEstimate(
            flops=6 * m * n * k, bytes_accessed=4 * m * k + 4 * k * n + 8 * m * n, transcendentals=0
        ),
        name="couple",
    )(ids, meta, whi, wlo, *pieces)


def finish_kernel(places, order_ref, meta_ref, base_ref, *refs):
    out_ref = refs[-1]
    row = meta_ref[0]
    y, x_lo, core = row // 4, row // 2 % 2, row % 2
    for i, chunk in enumerate(places):
        ours, theirs = refs[2 * i], refs[2 * i + 1]
        for j, (dy, lx, k) in enumerate(chunk):
            stored = (y + dy) % 4 * 4 + (x_lo + lx) % 2 * 2 + (core + k) % 2
            at = pl.ds(pl.multiple_of(order_ref[stored] * 128, 128), 128)
            cols = slice(j * 128, (j + 1) * 128)
            out_ref[:, at] = base_ref[:, at] - (ours[:, cols] + theirs[:, cols])


def finish(order, meta, base, places, sums):
    return pl.pallas_call(
        lambda *refs: finish_kernel(places, *refs),
        in_specs=[SMEM, SMEM] + [VMEM] * (1 + len(sums)),
        out_specs=VMEM,
        out_shape=jax.ShapeDtypeStruct(base.shape, F32),
        name="finish",
    )(order, meta, base, *sums)


def send(x, axis, pairs):
    return lax.ppermute(x, axis, pairs)


CHUNKS = (
    ((0, 0),),
    ((0, 1), (3, 0)),
    ((1, 0), (3, 1)),
    ((1, 1), (2, 0)),
    ((2, 1),),
)


def per_device(
    lower_inverse, upper_inverse, left_coupling, right_pieces, interface_block, a_gg, panel_order
):
    ids = interface_block[0, 0]
    meta = jnp.stack([lax.axis_index("row"), lax.axis_index("col")]).astype(jnp.int32)
    own = right_pieces[0]

    got = {(0, 0): own}
    got[0, 1] = send(own, "row", XLO)
    got[3, 0] = send(own, "row", yshift(1))
    got[1, 0] = send(own, "row", yshift(-1))
    got[3, 1] = send(got[0, 1], "row", yshift(1))
    got[1, 1] = send(got[0, 1], "row", yshift(-1))
    got[2, 0] = send(got[3, 0], "row", yshift(1))
    got[2, 1] = send(got[1, 1], "row", yshift(-1))
    sibling = {key: send(piece, "row", CORE) for key, piece in got.items()}

    whi, wlo = weights(left_coupling[0, 0], upper_inverse[0, 0], lower_inverse[0, 0])

    places, sums = [], []
    for chunk in CHUNKS:
        pieces = [from_[key] for key in chunk for from_ in (got, sibling)]
        places.append([(*key, k) for key in chunk for k in (0, 1)])
        a = couple(ids, meta, whi, wlo, pieces)
        near, far = a[:4], a[4:]
        far_near = send(near[2], "col", zshift(1))
        far_far = send(far[2], "col", zshift(-1))
        right_far = send(far[1], "col", zshift(1))
        left_near = send(near[3], "col", zshift(-1))
        right_near = send(near[1] + far_near, "col", zshift(1))
        left_far = send(far[3] + far_far, "col", zshift(-1))
        theirs = send(far[0] + right_far + left_far, "col", XHI)
        ours = near[0] + right_near + left_near
        sums += [ours, theirs]

    return finish(panel_order, meta, a_gg[0], places, sums)[None]


def solution(mesh):
    return jax.shard_map(
        per_device,
        mesh=mesh,
        in_specs=(
            P("row", "col", None, None),
            P("row", "col", None, None),
            P("row", "col", None, None),
            P("col", None, "row"),
            P("row", "col", None),
            P("row", "col", None),
            P(),
        ),
        out_specs=P("row", "col", None),
        check_vma=False,
    )
```

```python
import jax
import jax.numpy as jnp
from jax import lax
from jax.experimental import pallas as pl
from jax.experimental.pallas import tpu as pltpu
from jax.sharding import PartitionSpec as P

F32 = jnp.float32
BF16 = jnp.bfloat16

CORE = [(r, r ^ 1) for r in range(16)]
XLO = [(r, r ^ 2) for r in range(16)]
XHI = [(c, c ^ 4) for c in range(8)]


def yshift(d):
    return [(r, ((r // 4 + d) % 4) * 4 + r % 4) for r in range(16)]


def zshift(d):
    return [(c, (c // 4) * 4 + (c % 4 + d) % 4) for c in range(8)]


def split(x):
    hi = x.astype(BF16)
    return hi, (x - hi.astype(F32)).astype(BF16)


def mm(a, b):
    return jnp.dot(a, b, preferred_element_type=F32)


VMEM = pl.BlockSpec(memory_space=pltpu.VMEM)
SMEM = pl.BlockSpec(memory_space=pltpu.SMEM)


def weights_kernel(steps, left_ref, upper_ref, lower_ref, whi_ref, wlo_ref, thi, tlo):
    step = pl.program_id(0)
    width = upper_ref.shape[1]
    for j in range(steps):

        @pl.when(step == j)
        def _(j=j):
            depth = (j + 1) * width
            uhi, ulo = split(upper_ref[0:depth, :])
            left = left_ref[:, 0:depth]
            t = mm(left, uhi) + mm(left, ulo)
            hi, lo = split(t)
            thi[:, j * width : (j + 1) * width] = hi
            tlo[:, j * width : (j + 1) * width] = lo

        @pl.when(step == steps + j)
        def _(j=j):
            lhi, llo = split(lower_ref[j * width :, :])
            ahi = thi[:, j * width :]
            w = mm(ahi, lhi) + mm(ahi, llo) + mm(tlo[:, j * width :], lhi)
            hi, lo = split(w)
            whi_ref[:, j * width : (j + 1) * width] = hi
            wlo_ref[:, j * width : (j + 1) * width] = lo


def weights(left, upper, lower):
    m, n = left.shape
    steps = 4
    width = n // steps
    shape = jax.ShapeDtypeStruct((m, n), BF16)
    return pl.pallas_call(
        lambda *refs: weights_kernel(steps, *refs),
        grid=(2 * steps,),
        in_specs=[
            pl.BlockSpec((m, n), lambda s: (0, 0)),
            pl.BlockSpec((n, width), lambda s: (0, jnp.minimum(s, steps - 1))),
            pl.BlockSpec((n, width), lambda s: (0, jnp.maximum(s - steps, 0))),
        ],
        out_specs=[pl.BlockSpec((m, n), lambda s: (0, 0))] * 2,
        out_shape=[shape, shape],
        scratch_shapes=[pltpu.VMEM((m, n), BF16)] * 2,
        cost_estimate=pl.CostEstimate(
            flops=6 * m * n * n, bytes_accessed=8 * n * n + 6 * m * n, transcendentals=0
        ),
        compiler_params=pltpu.CompilerParams(vmem_limit_bytes=20 * 2**20),
        name="weights",
    )(left, upper, lower)


def couple_kernel(count, ids_ref, meta_ref, whi_ref, wlo_ref, *refs):
    pieces, outs, scratch = refs[:count], refs[count:-1], refs[-1]
    width = pieces[0].shape[1]
    his, los = zip(*(split(p[...]) for p in pieces))
    hi = jnp.concatenate(his, axis=1)
    lo = jnp.concatenate(los, axis=1)
    whi = whi_ref[...]
    scratch[...] = mm(whi, hi) + mm(whi, lo) + mm(wlo_ref[...], hi)
    col = meta_ref[1]
    x_hi, z = col // 4, col % 4
    for dx in range(2):
        for dz in range(4):
            out = outs[dx * 4 + dz]
            target = (x_hi + dx) % 2 * 4 + (z + dz) % 4
            source = jnp.int32(-1)
            for k in range(4):
                source = jnp.where(ids_ref[k] == target, jnp.int32(k), source)

            @pl.when(source >= 0)
            def _():
                rows = out.shape[0]
                out[...] = scratch[pl.ds(pl.multiple_of(source * rows, rows), rows), :]

            @pl.when(source < 0)
            def _():
                out[...] = jnp.zeros_like(out)


def couple(ids, meta, whi, wlo, pieces):
    m, k = whi.shape
    n = sum(p.shape[1] for p in pieces)
    shape = jax.ShapeDtypeStruct((m // 4, n), F32)
    return pl.pallas_call(
        lambda *refs: couple_kernel(len(pieces), *refs),
        in_specs=[SMEM, SMEM] + [VMEM] * (2 + len(pieces)),
        out_specs=[VMEM] * 8,
        out_shape=[shape] * 8,
        scratch_shapes=[pltpu.VMEM((m, n), F32)],
        cost_estimate=pl.CostEstimate(
            flops=6 * m * n * k, bytes_accessed=4 * m * k + 4 * k * n + 8 * m * n, transcendentals=0
        ),
        compiler_params=pltpu.CompilerParams(vmem_limit_bytes=14 * 2**20),
        name="couple",
    )(ids, meta, whi, wlo, *pieces)


def finish_kernel(places, order_ref, meta_ref, base_ref, *refs):
    out_ref = refs[-1]
    row = meta_ref[0]
    y, x_lo, core = row // 4, row // 2 % 2, row % 2
    for i, chunk in enumerate(places):
        ours, theirs = refs[2 * i], refs[2 * i + 1]
        for j, (dy, lx, k) in enumerate(chunk):
            stored = (y + dy) % 4 * 4 + (x_lo + lx) % 2 * 2 + (core + k) % 2
            at = pl.ds(pl.multiple_of(order_ref[stored] * 128, 128), 128)
            cols = slice(j * 128, (j + 1) * 128)
            out_ref[:, at] = base_ref[:, at] - (ours[:, cols] + theirs[:, cols])


def finish(order, meta, base, places, sums):
    return pl.pallas_call(
        lambda *refs: finish_kernel(places, *refs),
        in_specs=[SMEM, SMEM] + [VMEM] * (1 + len(sums)),
        out_specs=VMEM,
        out_shape=jax.ShapeDtypeStruct(base.shape, F32),
        compiler_params=pltpu.CompilerParams(vmem_limit_bytes=8 * 2**20),
        name="finish",
    )(order, meta, base, *sums)


def send(x, axis, pairs):
    return lax.ppermute(x, axis, pairs)


CHUNKS = (
    ((0, 0),),
    ((0, 1), (3, 0)),
    ((1, 0), (3, 1)),
    ((1, 1), (2, 0)),
    ((2, 1),),
)


def per_device(
    lower_inverse, upper_inverse, left_coupling, right_pieces, interface_block, a_gg, panel_order
):
    ids = interface_block[0, 0]
    meta = jnp.stack([lax.axis_index("row"), lax.axis_index("col")]).astype(jnp.int32)
    own = right_pieces[0]

    got = {(0, 0): own}
    got[0, 1] = send(own, "row", XLO)
    got[3, 0] = send(own, "row", yshift(1))
    got[1, 0] = send(own, "row", yshift(-1))
    got[3, 1] = send(got[0, 1], "row", yshift(1))
    got[1, 1] = send(got[0, 1], "row", yshift(-1))
    got[2, 0] = send(got[3, 0], "row", yshift(1))
    got[2, 1] = send(got[1, 1], "row", yshift(-1))
    sibling = {key: send(piece, "row", CORE) for key, piece in got.items()}

    whi, wlo = weights(left_coupling[0, 0], upper_inverse[0, 0], lower_inverse[0, 0])

    places, sums = [], []
    for chunk in CHUNKS:
        pieces = [from_[key] for key in chunk for from_ in (got, sibling)]
        places.append([(*key, k) for key in chunk for k in (0, 1)])
        a = couple(ids, meta, whi, wlo, pieces)
        near, far = a[:4], a[4:]
        far_near = send(near[2], "col", zshift(1))
        far_far = send(far[2], "col", zshift(-1))
        right_far = send(far[1], "col", zshift(1))
        left_near = send(near[3], "col", zshift(-1))
        right_near = send(near[1] + far_near, "col", zshift(1))
        left_far = send(far[3] + far_far, "col", zshift(-1))
        theirs = send(far[0] + right_far + left_far, "col", XHI)
        ours = near[0] + right_near + left_near
        sums += [ours, theirs]

    return finish(panel_order, meta, a_gg[0], places, sums)[None]


def solution(mesh):
    return jax.shard_map(
        per_device,
        mesh=mesh,
        in_specs=(
            P("row", "col", None, None),
            P("row", "col", None, None),
            P("row", "col", None, None),
            P("col", None, "row"),
            P("row", "col", None),
            P("row", "col", None),
            P(),
        ),
        out_specs=P("row", "col", None),
        check_vma=False,
    )
```
